32 devices in a mesh: pairs: 16 (over z, y, x), side: 2 (over core).
Axes of the slice: x: 2, y: 2, z: 4, core: 2. Of those that a mesh axis runs over, the one named last changes fastest.
Arguments:
- features: bfloat16 [16, 196, 768], P('pairs', None, 'side'), may hold values from -6 to 6
- image_slot: int32 [16], replicated, may hold values from 0 to 15, as said below
- slot_images: int32 [48, 2], P('pairs'), may hold values from 0 to 15, as said below
- slot_count: int32 [16], P('pairs'), may hold values from 1 to 3, as said below
- gain_self: float32 [2, 768], P('side'), may hold values from 0.5 to 1.5
- gain_query: float32 [2, 768], P('side'), may hold values from 0.5 to 1.5
- gain_memory: float32 [2, 768], P('side'), may hold values from 0.5 to 1.5
- gain_mlp: float32 [2, 768], P('side'), may hold values from 0.5 to 1.5
- gain_head: float32 [2, 768], P('side'), may hold values from 0.5 to 1.5
- w_qkv: bfloat16 [2, 768, 2304], P('side'), may hold values from -0.21875 to 0.21875
- w_self_out: bfloat16 [2, 768, 768], P('side'), may hold values from -0.21875 to 0.21875
- w_query: bfloat16 [2, 768, 768], P('side'), may hold values from -0.21875 to 0.21875
- w_memory: bfloat16 [2, 768, 1536], P('side'), may hold values from -0.21875 to 0.21875
- w_cross_out: bfloat16 [2, 768, 768], P('side'), may hold values from -0.21875 to 0.21875
- w_fc1: bfloat16 [2, 3072, 768], P('side', 'pairs'), may hold values from -0.21875 to 0.21875
- w_fc2: bfloat16 [2, 3072, 768], P('side', 'pairs'), may hold values from -0.109375 to 0.109375
- w_head: bfloat16 [2, 768, 1024], P('side'), may hold values from -0.21875 to 0.21875
Outputs:
- merged_points: bfloat16 [16, 196, 768], P('pairs', None, 'side')
The draws below stay inside these ranges and needn't reach their ends.
Inputs may be any that keep to these rules, and one draw needn't show every extreme that they name: A permutation: image i is storage row image_slot[i] of features, held by device image_slot[i] // 1 of pairs. `slot_images`: slot j belongs to device j // 3 of pairs; its two images are distinct, and each is held by device (j // 3 + k) mod the size of pairs for some 0 <= k < 4; k = 3 occurs. `slot_count`: the counts sum to 32; 3 is reached on a quarter of the devices.
All inputs are finite; a program needn't handle non-finite values.
Results may differ from the reference program's by a relative error of at most 0.015.
Values may be sent and summed in bfloat16 or wider, within the bound.
A program may use at most 128 MiB of HBM per device.

```python
import jax
import jax.numpy as jnp
from jax import lax

D = 768
HEADS = 12
FF = 3072
HEAD_DIM = 64
TOKI = 196
PIXELS = 256
WINDOW = 4
IMG_DEV = 1
PAIR_DEV = 2
PAIR_MAX = 3
IMAGES = 16
SLOTS = 48


def routing_tables(key):
    n_dev = IMAGES // IMG_DEV
    keys = jax.random.split(jax.random.fold_in(key, 31), 4)
    image_slot = jax.random.permutation(keys[0], IMAGES).astype(jnp.int32)
    row_image = jnp.zeros((IMAGES,), jnp.int32).at[image_slot].set(jnp.arange(IMAGES, dtype=jnp.int32))
    order = jax.random.permutation(keys[1], n_dev).astype(jnp.int32)
    ranking = jnp.zeros((n_dev,), jnp.int32).at[order].set(jnp.arange(n_dev, dtype=jnp.int32))
    quarter = n_dev // 4
    halfway = PAIR_DEV // 2
    counts = PAIR_DEV + jnp.where(ranking < quarter, halfway, 0) - jnp.where((ranking >= quarter) & (ranking < 2 * quarter), halfway, 0)
    offsets = jax.random.randint(keys[2], (SLOTS, 2), 0, WINDOW).astype(jnp.int32)
    offsets = offsets.at[0, 0].set(WINDOW - 1)
    within = jax.random.randint(keys[3], (SLOTS, 2), 0, IMG_DEV).astype(jnp.int32)
    clash = (offsets[:, 0] == offsets[:, 1]) & (within[:, 0] == within[:, 1])
    second = jnp.where(clash, (offsets[:, 1] + 1) % WINDOW, offsets[:, 1])
    offsets = jnp.stack([offsets[:, 0], second], axis=1)
    device = (jnp.arange(SLOTS, dtype=jnp.int32) // PAIR_MAX)[:, None]
    holder = (device + offsets) % n_dev
    slot_images = row_image[holder * IMG_DEV + within]
    return (image_slot, slot_images.astype(jnp.int32), counts.astype(jnp.int32))


def draw_image_slot(key, part):
    return routing_tables(key)[0]


def draw_slot_images(key, part):
    return routing_tables(key)[1]


def draw_slot_count(key, part):
    return routing_tables(key)[2]


def shard_levels(stream_key, dims, pieces, least, top_value):
    loudness = 1.0
    for dim, blocks in pieces:
        draws = jax.random.uniform(jax.random.fold_in(jax.random.fold_in(stream_key, 6), dim), (blocks,), jnp.float32, least / len(pieces), top_value / len(pieces))
        loudness = loudness * jnp.repeat(jnp.exp(draws), dims[dim] // blocks).reshape((-1,) + (1,) * (len(dims) - 1 - dim))
    return loudness


def bell_draw(rng, extent, width, limit, cuts=(), kind=jnp.bfloat16):
    entries = width * jax.random.normal(rng, extent, jnp.float32)
    if cuts:
        entries = entries * shard_levels(rng, extent, cuts, -0.22, 0.18)
    return jnp.clip(entries, -limit, limit).astype(kind)


def setup_inputs(seed: int = 0) -> dict:
    key_list = jax.random.split(jax.random.key(seed), 18)
    features = bell_draw(key_list[0], (IMAGES, TOKI, D), 1.0, 6.0, ((0, 16), (2, 2)))
    image_slot = draw_image_slot(jax.random.fold_in(key_list[17], 71), 0)
    slot_images = draw_slot_images(jax.random.fold_in(key_list[17], 71), 0)
    slot_count = draw_slot_count(jax.random.fold_in(key_list[17], 71), 0)
    gain_self = jnp.clip(1.0 + 0.1 * jax.random.normal(key_list[4], (2, D), jnp.float32), 0.5, 1.5)
    gain_query = jnp.clip(1.0 + 0.1 * jax.random.normal(key_list[5], (2, D), jnp.float32), 0.5, 1.5)
    gain_memory = jnp.clip(1.0 + 0.1 * jax.random.normal(key_list[6], (2, D), jnp.float32), 0.5, 1.5)
    gain_mlp = jnp.clip(1.0 + 0.1 * jax.random.normal(key_list[7], (2, D), jnp.float32), 0.5, 1.5)
    gain_head = jnp.clip(1.0 + 0.1 * jax.random.normal(key_list[8], (2, D), jnp.float32), 0.5, 1.5)
    w_qkv = bell_draw(key_list[9], (2, D, 3 * D), D ** -0.5, 0.21875, ((0, 2),))
    w_self_out = bell_draw(key_list[10], (2, D, D), D ** -0.5, 0.21875, ((0, 2),))
    w_query = bell_draw(key_list[11], (2, D, D), D ** -0.5, 0.21875, ((0, 2),))
    w_memory = bell_draw(key_list[12], (2, D, 2 * D), D ** -0.5, 0.21875, ((0, 2),))
    w_cross_out = bell_draw(key_list[13], (2, D, D), D ** -0.5, 0.21875, ((0, 2),))
    w_fc1 = bell_draw(key_list[14], (2, FF, D), D ** -0.5, 0.21875, ((0, 2), (1, 16)))
    w_fc2 = bell_draw(key_list[15], (2, FF, D), FF ** -0.5, 0.109375, ((0, 2), (1, 16)))
    w_head = bell_draw(key_list[16], (2, D, 4 * PIXELS), D ** -0.5, 0.21875, ((0, 2),))
    return dict(features=features, image_slot=image_slot, slot_images=slot_images, slot_count=slot_count, gain_self=gain_self, gain_query=gain_query, gain_memory=gain_memory, gain_mlp=gain_mlp, gain_head=gain_head, w_qkv=w_qkv, w_self_out=w_self_out, w_query=w_query, w_memory=w_memory, w_cross_out=w_cross_out, w_fc1=w_fc1, w_fc2=w_fc2, w_head=w_head)


def layer_norm(values, gain):
    center = values - lax.optimization_barrier(jnp.mean(values, axis=-1, keepdims=True))
    spread = lax.optimization_barrier(jnp.mean(center * center, axis=-1, keepdims=True))
    return center * lax.rsqrt(spread + 1e-06) * gain

def attend(queries, key_rows, value_rows):
    length = queries.shape[0]
    key_len = key_rows.shape[0]
    q_heads = queries.astype(jnp.float32).reshape(length, HEADS, HEAD_DIM)
    k_heads = key_rows.astype(jnp.float32).reshape(key_len, HEADS, HEAD_DIM)
    v_heads = value_rows.astype(jnp.float32).reshape(key_len, HEADS, HEAD_DIM)
    scores = jnp.einsum('qhd,khd->hqk', q_heads, k_heads) * HEAD_DIM ** (-0.5)
    expon = jnp.exp(scores)
    weights = (expon / lax.optimization_barrier(jnp.sum(expon, axis=-1, keepdims=True))).astype(jnp.bfloat16)
    mixed = jnp.einsum('hqk,khd->qhd', weights.astype(jnp.float32), v_heads)
    return mixed.astype(jnp.bfloat16).reshape(length, D)

def decode(tokens, memory, gains, mats):
    g_self, g_query, g_memory, g_mlp, g_head = gains
    m_qkv, m_self_out, m_query, m_memory, m_cross_out, m_fc_in, m_fc_out, m_head = mats
    hidden = layer_norm(tokens.astype(jnp.float32), g_self).astype(jnp.bfloat16)
    triple = jnp.dot(hidden, m_qkv, preferred_element_type=jnp.float32).astype(jnp.bfloat16)
    attended = attend(triple[:, :D], triple[:, D:2 * D], triple[:, 2 * D:])
    first = tokens.astype(jnp.float32) + jnp.dot(attended, m_self_out, preferred_element_type=jnp.float32)
    query_in = layer_norm(first, g_query).astype(jnp.bfloat16)
    memory_in = layer_norm(memory.astype(jnp.float32), g_memory).astype(jnp.bfloat16)
    queries = jnp.dot(query_in, m_query, preferred_element_type=jnp.float32).astype(jnp.bfloat16)
    key_value = jnp.dot(memory_in, m_memory, preferred_element_type=jnp.float32).astype(jnp.bfloat16)
    crossed = attend(queries, key_value[:, :D], key_value[:, D:])
    second = first + jnp.dot(crossed, m_cross_out, preferred_element_type=jnp.float32)
    mlp_in = layer_norm(second, g_mlp).astype(jnp.bfloat16)
    pre_act = jnp.dot(mlp_in, m_fc_in.T, preferred_element_type=jnp.float32)
    activated = jax.nn.gelu(pre_act, approximate=False).astype(jnp.bfloat16)
    third = second + jnp.dot(activated, m_fc_out, preferred_element_type=jnp.float32)
    final = layer_norm(third, g_head).astype(jnp.bfloat16)
    return jnp.dot(final, m_head, preferred_element_type=jnp.float32)

def map_terms(raw):
    lead = raw.shape[:-1]
    parts = raw.reshape(lead + (2, 4, PIXELS // 2))
    conf = 1.0 + jnp.exp(parts[..., 3, :])
    joined = jnp.concatenate([conf[..., None, :] * parts[..., :3, :], conf[..., None, :]], axis=-2)
    return joined.reshape(lead + (4 * PIXELS,))

def reference(features, image_slot, slot_images, slot_count, gain_self, gain_query, gain_memory, gain_mlp, gain_head, w_qkv, w_self_out, w_query, w_memory, w_cross_out, w_fc1, w_fc2, w_head):
    gain_list = [gain_self, gain_query, gain_memory, gain_mlp, gain_head]
    mat_list = [w_qkv, w_self_out, w_query, w_memory, w_cross_out, w_fc1, w_fc2, w_head]

    def one_slot(sums, index):
        live = (index % PAIR_MAX < slot_count[index // PAIR_MAX]).astype(jnp.float32)
        stored = image_slot[slot_images[index]].astype(jnp.int32)
        views = [lax.dynamic_index_in_dim(features, stored[which], 0, keepdims=False) for which in range(2)]
        for which in range(2):
            result = decode(views[which], views[1 - which], [g[which] for g in gain_list], [m[which] for m in mat_list])
            sums = sums.at[stored[which]].add(live * map_terms(result))
        return (sums, None)
    start = jnp.zeros((IMAGES, TOKI, 4 * PIXELS), jnp.float32)
    sums, _ = lax.scan(one_slot, start, jnp.arange(SLOTS, dtype=jnp.int32))
    parts = sums.reshape(IMAGES, TOKI, 2, 4, PIXELS // 2)
    merged = parts[:, :, :, :3] / jnp.maximum(parts[:, :, :, 3:], 1.0)
    return merged.reshape(IMAGES, TOKI, 3 * PIXELS).astype(jnp.bfloat16)
```

```python
import functools

import jax
import jax.numpy as jnp
from jax import lax
from jax.experimental import pallas as pl
from jax.experimental.pallas import tpu as pltpu
from jax.sharding import PartitionSpec as P

HEAD_DIM = 64
WINDOW = 4
PAIR = 2 * HEAD_DIM
VMEM_LIMIT = 60 * 1024 * 1024


def padded(rows):
    return -(-rows // 16) * 16


def layer_norm(values, gain):
    center = values - jnp.mean(values, axis=-1, keepdims=True)
    spread = jnp.mean(center * center, axis=-1, keepdims=True)
    return center * lax.rsqrt(spread + 1e-06) * gain


def matmul(left, right):
    return jnp.dot(left, right, preferred_element_type=jnp.float32)


def attend(q_ref, k_ref, v_ref, q_at, k_at, v_at, o_ref, width):
    rows = q_ref.shape[0]
    low = lax.broadcasted_iota(jnp.int32, (rows, PAIR), 1) < HEAD_DIM
    for pair in range(width // PAIR):
        q = q_ref[:, q_at + pair * PAIR : q_at + (pair + 1) * PAIR]
        k = k_ref[:, k_at + pair * PAIR : k_at + (pair + 1) * PAIR]
        v = v_ref[:, v_at + pair * PAIR : v_at + (pair + 1) * PAIR]
        mixed = None
        for keep in (low, jnp.logical_not(low)):
            q_head = jnp.where(keep, q, jnp.zeros_like(q))
            v_head = jnp.where(keep, v, jnp.zeros_like(v))
            scores = lax.dot_general(
                q_head, k, (((1,), (1,)), ((), ())), preferred_element_type=jnp.float32
            ) * HEAD_DIM ** (-0.5)
            expon = jnp.exp(scores)
            weights = (expon / jnp.sum(expon, axis=-1, keepdims=True)).astype(jnp.bfloat16)
            part = matmul(weights, v_head)
            mixed = part if mixed is None else mixed + part
        o_ref[:, pair * PAIR : (pair + 1) * PAIR] = mixed.astype(jnp.bfloat16)


def front_kernel(
    which, window, g_self, g_query, g_memory, g_mlp, m_qkv, m_self_out, m_query, m_memory,
    m_cross_out, second_out, mlp_in_out, triple, kv, queries, mixed
):
    rows, width = window.shape[1], window.shape[2]
    tokens = window[which[0]].astype(jnp.float32)
    hidden = layer_norm(tokens, g_self[...]).astype(jnp.bfloat16)
    triple[...] = matmul(hidden, m_qkv[...]).astype(jnp.bfloat16)
    attend(triple, triple, triple, 0, width, 2 * width, mixed, width)
    first = tokens + matmul(mixed[...], m_self_out[...])
    query_in = layer_norm(first, g_query[...]).astype(jnp.bfloat16)
    memory_in = layer_norm(window[which[1]].astype(jnp.float32), g_memory[...]).astype(jnp.bfloat16)
    queries[...] = matmul(query_in, m_query[...]).astype(jnp.bfloat16)
    kv[...] = matmul(memory_in, m_memory[...]).astype(jnp.bfloat16)
    attend(queries, kv, kv, 0, 0, width, mixed, width)
    second = first + matmul(mixed[...], m_cross_out[...])
    mlp_in_out[...] = jnp.zeros_like(mlp_in_out)
    second_out[...] = jnp.zeros_like(second_out)
    second_out[0:rows, :] = second
    mlp_in_out[0:rows, :] = layer_norm(second, g_mlp[...]).astype(jnp.bfloat16)


def front(which, window, gains, mats):
    rows, width = window.shape[1], window.shape[2]
    tall = padded(rows)
    flops = 2 * rows * width * width * 8 + 8 * rows * rows * width
    return pl.pallas_call(
        front_kernel,
        out_shape=(
            jax.ShapeDtypeStruct((tall, width), jnp.float32),
            jax.ShapeDtypeStruct((tall, width), jnp.bfloat16),
        ),
        in_specs=[pl.BlockSpec(memory_space=pltpu.SMEM)]
        + [pl.BlockSpec(memory_space=pltpu.VMEM)] * (1 + len(gains) + len(mats)),
        out_specs=(pl.BlockSpec(memory_space=pltpu.VMEM),) * 2,
        scratch_shapes=[
            pltpu.VMEM((rows, 3 * width), jnp.bfloat16),
            pltpu.VMEM((rows, 2 * width), jnp.bfloat16),
            pltpu.VMEM((rows, width), jnp.bfloat16),
            pltpu.VMEM((rows, width), jnp.bfloat16),
        ],
        compiler_params=pltpu.CompilerParams(vmem_limit_bytes=VMEM_LIMIT),
        cost_estimate=pl.CostEstimate(
            flops=8 * flops, bytes_accessed=20 * width * width, transcendentals=0
        ),
    )(which, window, *gains, *mats)


def back_kernel(slots, rows, own_index, count, side, *refs):
    seconds, mlp_ins = refs[:slots], refs[slots : 2 * slots]
    pieces = refs[2 * slots : 2 * slots + 4]
    g_head, m_head, keep_out, send_out, inp, acc = refs[2 * slots + 4 :]
    tall = padded(rows)
    for slot in range(slots):
        inp[slot * tall : (slot + 1) * tall, :] = mlp_ins[slot][...]
        acc[slot * tall : (slot + 1) * tall, :] = seconds[slot][...]
    step = 256
    for piece in pieces:

        def block(at, carry, piece=piece):
            where = pl.ds(pl.multiple_of(at * step, step), step)
            pre = lax.dot_general(
                inp[...], piece[0, where, :], (((1,), (1,)), ((), ())),
                preferred_element_type=jnp.float32,
            )
            act = (pre * (1.0 + lax.erf(pre * 0.5**0.5)) * 0.5).astype(jnp.bfloat16)
            acc[...] += matmul(act, piece[1, where, :])
            return carry

        lax.fori_loop(0, piece.shape[1] // step, block, 0)
    half = m_head.shape[1] // 2
    pix = half // 4
    for out in (keep_out, send_out):
        out[...] = jnp.zeros_like(out)
    final = layer_norm(acc[...], g_head[...]).astype(jnp.bfloat16)
    inp[...] = final
    for part in range(2):
        raw = matmul(inp[...], m_head[:, part * half : (part + 1) * half])
        conf = 1.0 + jnp.exp(raw[:, 3 * pix :])
        for comp in range(4):
            term = conf if comp == 3 else conf * raw[:, comp * pix : (comp + 1) * pix]
            for w in range(keep_out.shape[0]):
                total = jnp.zeros((tall, pix), jnp.float32)
                for slot in range(slots):
                    chosen = jnp.logical_and(own_index[slot] == w, slot < count[0])
                    total = total + jnp.where(chosen, term[slot * tall : (slot + 1) * tall], 0.0)
                total = total[0:rows]
                at = slice(comp * pix, (comp + 1) * pix)

                @pl.when(side[0] == part)
                def _(total=total, w=w, at=at):
                    keep_out[w, :, at] = total

                @pl.when(side[0] != part)
                def _(total=total, w=w, at=at):
                    send_out[w, :, at] = total.astype(jnp.bfloat16)


def back(own_index, count, side, seconds, mlp_ins, pieces, g_head, m_head, rows, windows):
    slots = len(seconds)
    tall, width = seconds[0].shape
    half = m_head.shape[1] // 2
    return pl.pallas_call(
        functools.partial(back_kernel, slots, rows),
        out_shape=(
            jax.ShapeDtypeStruct((windows, rows, half), jnp.float32),
            jax.ShapeDtypeStruct((windows, rows, half), jnp.bfloat16),
        ),
        in_specs=[pl.BlockSpec(memory_space=pltpu.SMEM)] * 3
        + [pl.BlockSpec(memory_space=pltpu.VMEM)] * (2 * slots + 4 + 2),
        out_specs=(pl.BlockSpec(memory_space=pltpu.VMEM),) * 2,
        scratch_shapes=[
            pltpu.VMEM((slots * tall, width), jnp.bfloat16),
            pltpu.VMEM((slots * tall, width), jnp.float32),
        ],
        compiler_params=pltpu.CompilerParams(vmem_limit_bytes=VMEM_LIMIT),
    )(own_index, count, side, *seconds, *mlp_ins, *pieces, g_head, m_head)


def passed_along(array, axis, by):
    count = lax.axis_size(axis)
    return lax.ppermute(array, axis, [(i, (i + by) % count) for i in range(count)])


def doubled(block, bits):
    count = lax.axis_size("pairs")
    for bit in bits:
        other = lax.ppermute(block, "pairs", [(i, i ^ bit) for i in range(count)])
        if bit == bits[-1]:
            return [block, other]
        block = jnp.concatenate([block, other], axis=1)


def on_device(
    features, image_slot, slot_images, slot_count, gain_self, gain_query, gain_memory, gain_mlp,
    gain_head, w_qkv, w_self_out, w_query, w_memory, w_cross_out, w_fc1, w_fc2, w_head,
):
    devices = lax.axis_size("pairs")
    here = lax.axis_index("pairs")
    side = lax.axis_index("side")
    img_local, rows = features.shape[0], features.shape[1]
    slots = slot_images.shape[0]
    stored = image_slot[slot_images]
    index = (stored // img_local - here) % devices * img_local + stored % img_local
    which = jnp.where(side == 0, index, index[:, ::-1]).astype(jnp.int32)

    units = w_fc1.shape[1]
    cut = units // 2
    both = jnp.concatenate([w_fc1, w_fc2], axis=0)
    high = [1 << b for b in reversed(range(2, devices.bit_length() - 1))]
    chain_a = doubled(both[:, :cut], high + [1, 2])
    chain_b = doubled(both[:, cut:], high + [2, 1])

    blocks = [features] + [passed_along(features, "pairs", -by) for by in range(1, WINDOW)]
    mine = jnp.concatenate(blocks, axis=0)
    other = passed_along(mine, "side", 1)
    window = jnp.concatenate(
        [jnp.where(side == 0, mine, other), jnp.where(side == 0, other, mine)], axis=-1
    )
    gains = [gain_self, gain_query, gain_memory, gain_mlp]
    mats = [w_qkv[0], w_self_out[0], w_query[0], w_memory[0], w_cross_out[0]]
    fronts = [front(which[slot], window, gains, mats) for slot in range(slots)]
    keep, send = back(
        which[:, 0], slot_count, side.astype(jnp.int32)[None], [f[0] for f in fronts],
        [f[1] for f in fronts], chain_a + chain_b, gain_head, w_head[0], rows, window.shape[0],
    )
    sums = keep + passed_along(send, "side", 1).astype(jnp.float32)
    total = sums[:img_local]
    for by in range(1, WINDOW):
        piece = sums[by * img_local : (by + 1) * img_local]
        total = total + passed_along(piece.astype(jnp.bfloat16), "pairs", by).astype(jnp.float32)
    coords = total.shape[-1] * 3 // 4
    pix = total.shape[-1] // 4
    conf = jnp.maximum(total[:, :, coords:], 1.0)
    merged = [total[:, :, c * pix : (c + 1) * pix] / conf for c in range(3)]
    return jnp.concatenate(merged, axis=-1).astype(jnp.bfloat16)


def solution(mesh):
    placed = (
        P("pairs", None, "side"),
        P(),
        P("pairs", None),
        P("pairs"),
        P("side", None),
        P("side", None),
        P("side", None),
        P("side", None),
        P("side", None),
        P("side", None, None),
        P("side", None, None),
        P("side", None, None),
        P("side", None, None),
        P("side", None, None),
        P("side", "pairs", None),
        P("side", "pairs", None),
        P("side", None, None),
    )
    return jax.shard_map(
        on_device, mesh=mesh, in_specs=placed, out_specs=P("pairs", None, "side"), check_vma=False
    )
```

```python
import functools

import jax
import jax.numpy as jnp
from jax import lax
from jax.experimental import pallas as pl
from jax.experimental.pallas import tpu as pltpu
from jax.sharding import PartitionSpec as P

HEAD_DIM = 64
WINDOW = 4
GROUP = 4
PAIR = 2 * HEAD_DIM
VMEM_LIMIT = 60 * 1024 * 1024


def padded(rows):
    return -(-rows // 16) * 16


def layer_norm(values, gain):
    center = values - jnp.mean(values, axis=-1, keepdims=True)
    spread = jnp.mean(center * center, axis=-1, keepdims=True)
    return center * lax.rsqrt(spread + 1e-06) * gain


def matmul(left, right):
    return jnp.dot(left, right, preferred_element_type=jnp.float32)


def attend(q_ref, k_ref, v_ref, q_at, k_at, v_at, o_ref, width):
    rows = q_ref.shape[0]
    low = lax.broadcasted_iota(jnp.int32, (rows, PAIR), 1) < HEAD_DIM
    for pair in range(width // PAIR):
        q = q_ref[:, q_at + pair * PAIR : q_at + (pair + 1) * PAIR]
        k = k_ref[:, k_at + pair * PAIR : k_at + (pair + 1) * PAIR]
        v = v_ref[:, v_at + pair * PAIR : v_at + (pair + 1) * PAIR]
        mixed = None
        for keep in (low, jnp.logical_not(low)):
            q_head = jnp.where(keep, q, jnp.zeros_like(q))
            v_head = jnp.where(keep, v, jnp.zeros_like(v))
            scores = lax.dot_general(
                q_head, k, (((1,), (1,)), ((), ())), preferred_element_type=jnp.float32
            ) * HEAD_DIM ** (-0.5)
            expon = jnp.exp(scores)
            weights = (expon / jnp.sum(expon, axis=-1, keepdims=True)).astype(jnp.bfloat16)
            part = matmul(weights, v_head)
            mixed = part if mixed is None else mixed + part
        o_ref[:, pair * PAIR : (pair + 1) * PAIR] = mixed.astype(jnp.bfloat16)


def front_kernel(
    which, window, g_self, g_query, g_memory, g_mlp, m_qkv, m_self_out, m_query, m_memory,
    m_cross_out, second_out, mlp_in_out, triple, kv, queries, mixed
):
    rows, width = window.shape[1], window.shape[2]
    tokens = window[which[0]].astype(jnp.float32)
    hidden = layer_norm(tokens, g_self[...]).astype(jnp.bfloat16)
    triple[...] = matmul(hidden, m_qkv[...]).astype(jnp.bfloat16)
    attend(triple, triple, triple, 0, width, 2 * width, mixed, width)
    first = tokens + matmul(mixed[...], m_self_out[...])
    query_in = layer_norm(first, g_query[...]).astype(jnp.bfloat16)
    memory_in = layer_norm(window[which[1]].astype(jnp.float32), g_memory[...]).astype(jnp.bfloat16)
    queries[...] = matmul(query_in, m_query[...]).astype(jnp.bfloat16)
    kv[...] = matmul(memory_in, m_memory[...]).astype(jnp.bfloat16)
    attend(queries, kv, kv, 0, 0, width, mixed, width)
    second = first + matmul(mixed[...], m_cross_out[...])
    mlp_in_out[...] = jnp.zeros_like(mlp_in_out)
    second_out[...] = jnp.zeros_like(second_out)
    second_out[0:rows, :] = second
    mlp_in_out[0:rows, :] = layer_norm(second, g_mlp[...]).astype(jnp.bfloat16)


def front(which, window, gains, mats):
    rows, width = window.shape[1], window.shape[2]
    tall = padded(rows)
    flops = 2 * rows * width * width * 8 + 8 * rows * rows * width
    return pl.pallas_call(
        front_kernel,
        out_shape=(
            jax.ShapeDtypeStruct((tall, width), jnp.float32),
            jax.ShapeDtypeStruct((tall, width), jnp.bfloat16),
        ),
        in_specs=[pl.BlockSpec(memory_space=pltpu.SMEM)]
        + [pl.BlockSpec(memory_space=pltpu.VMEM)] * (1 + len(gains) + len(mats)),
        out_specs=(pl.BlockSpec(memory_space=pltpu.VMEM),) * 2,
        scratch_shapes=[
            pltpu.VMEM((rows, 3 * width), jnp.bfloat16),
            pltpu.VMEM((rows, 2 * width), jnp.bfloat16),
            pltpu.VMEM((rows, width), jnp.bfloat16),
            pltpu.VMEM((rows, width), jnp.bfloat16),
        ],
        compiler_params=pltpu.CompilerParams(vmem_limit_bytes=VMEM_LIMIT),
        cost_estimate=pl.CostEstimate(
            flops=8 * flops, bytes_accessed=20 * width * width, transcendentals=0
        ),
    )(which, window, *gains, *mats)


def mlp_kernel(group, *refs):
    inputs, pieces = refs[:group], refs[group : group + 2]
    outs, inp, acc = refs[group + 2 : 2 * group + 2], refs[-2], refs[-1]
    tall = inputs[0].shape[0]
    for at in range(group):
        inp[at * tall : (at + 1) * tall, :] = inputs[at][...]
    acc[...] = jnp.zeros_like(acc)
    step = 128
    for piece in pieces:

        def block(at, carry, piece=piece):
            where = pl.ds(pl.multiple_of(at * step, step), step)
            pre = lax.dot_general(
                inp[...], piece[0, where, :], (((1,), (1,)), ((), ())),
                preferred_element_type=jnp.float32,
            )
            act = (pre * (1.0 + lax.erf(pre * 0.5**0.5)) * 0.5).astype(jnp.bfloat16)
            acc[...] += matmul(act, piece[1, where, :])
            return carry

        lax.fori_loop(0, piece.shape[1] // step, block, 0)
    for at in range(group):
        outs[at][...] = acc[at * tall : (at + 1) * tall, :].astype(outs[at].dtype)


def mlp(inputs, pieces):
    group = len(inputs)
    tall, width = inputs[0].shape
    return pl.pallas_call(
        functools.partial(mlp_kernel, group),
        out_shape=tuple(
            jax.ShapeDtypeStruct((tall, width), jnp.float32 if at == 0 else jnp.bfloat16)
            for at in range(group)
        ),
        in_specs=[pl.BlockSpec(memory_space=pltpu.VMEM)] * (group + 2),
        out_specs=(pl.BlockSpec(memory_space=pltpu.VMEM),) * group,
        scratch_shapes=[
            pltpu.VMEM((group * tall, width), jnp.bfloat16),
            pltpu.VMEM((group * tall, width), jnp.float32),
        ],
        compiler_params=pltpu.CompilerParams(vmem_limit_bytes=VMEM_LIMIT // 2),
        cost_estimate=pl.CostEstimate(
            flops=24 * group * tall * width * pieces[0].shape[1] * 2,
            bytes_accessed=8 * group * tall * width,
            transcendentals=0,
        ),
    )(*inputs, *pieces)


def tail_kernel(slots, group, rows, own_index, count, side, *refs):
    parts = refs[: slots * (group + 1)]
    g_head, m_head, keep_out, send_out, final = refs[slots * (group + 1) :]
    tall = padded(rows)
    for slot in range(slots):
        third = None
        for ref in parts[slot * (group + 1) : (slot + 1) * (group + 1)]:
            value = ref[...].astype(jnp.float32)
            third = value if third is None else third + value
        final[slot * tall : (slot + 1) * tall, :] = layer_norm(third, g_head[...]).astype(
            jnp.bfloat16
        )
    half = m_head.shape[1] // 2
    pix = half // 4
    for part in range(2):
        raw = matmul(final[...], m_head[:, part * half : (part + 1) * half])
        conf = 1.0 + jnp.exp(raw[:, 3 * pix :])
        for comp in range(4):
            term = conf if comp == 3 else conf * raw[:, comp * pix : (comp + 1) * pix]
            for w in range(keep_out.shape[0]):
                total = jnp.zeros((tall, pix), jnp.float32)
                for slot in range(slots):
                    chosen = jnp.logical_and(own_index[slot] == w, slot < count[0])
                    total = total + jnp.where(chosen, term[slot * tall : (slot + 1) * tall], 0.0)
                total = total[0:rows]
                at = slice(comp * pix, (comp + 1) * pix)

                @pl.when(side[0] == part)
                def _(total=total, w=w, at=at):
                    keep_out[w, :, at] = total

                @pl.when(side[0] != part)
                def _(total=total, w=w, at=at):
                    send_out[w, :, at] = total.astype(jnp.bfloat16)


def tail(own_index, count, side, parts, g_head, m_head, rows, windows):
    slots = len(parts)
    tall, width = parts[0][0].shape
    half = m_head.shape[1] // 2
    flat = [ref for slot in parts for ref in slot]
    return pl.pallas_call(
        functools.partial(tail_kernel, slots, len(parts[0]) - 1, rows),
        out_shape=(
            jax.ShapeDtypeStruct((windows, rows, half), jnp.float32),
            jax.ShapeDtypeStruct((windows, rows, half), jnp.bfloat16),
        ),
        in_specs=[pl.BlockSpec(memory_space=pltpu.SMEM)] * 3
        + [pl.BlockSpec(memory_space=pltpu.VMEM)] * (len(flat) + 2),
        out_specs=(pl.BlockSpec(memory_space=pltpu.VMEM),) * 2,
        scratch_shapes=[pltpu.VMEM((slots * tall, width), jnp.bfloat16)],
        compiler_params=pltpu.CompilerParams(vmem_limit_bytes=VMEM_LIMIT // 2),
    )(own_index, count, side, *flat, g_head, m_head)


def crossed(array, bits):
    count = lax.axis_size("pairs")
    return lax.ppermute(array, "pairs", [(i, i ^ bits) for i in range(count)])


def passed_along(array, axis, by):
    count = lax.axis_size(axis)
    return lax.ppermute(array, axis, [(i, (i + by) % count) for i in range(count)])


def doubled(block, bits):
    count = lax.axis_size("pairs")
    for bit in bits:
        other = lax.ppermute(block, "pairs", [(i, i ^ bit) for i in range(count)])
        if bit == bits[-1]:
            return [block, other]
        block = jnp.concatenate([block, other], axis=1)


def on_device(
    features, image_slot, slot_images, slot_count, gain_self, gain_query, gain_memory, gain_mlp,
    gain_head, w_qkv, w_self_out, w_query, w_memory, w_cross_out, w_fc1, w_fc2, w_head,
):
    devices = lax.axis_size("pairs")
    here = lax.axis_index("pairs")
    side = lax.axis_index("side")
    img_local, rows = features.shape[0], features.shape[1]
    slots = slot_images.shape[0]
    stored = image_slot[slot_images]
    index = (stored // img_local - here) % devices * img_local + stored % img_local
    which = jnp.where(side == 0, index, index[:, ::-1]).astype(jnp.int32)

    blocks = [features] + [passed_along(features, "pairs", -by) for by in range(1, WINDOW)]
    mine = jnp.concatenate(blocks, axis=0)
    other = passed_along(mine, "side", 1)
    window = jnp.concatenate(
        [jnp.where(side == 0, mine, other), jnp.where(side == 0, other, mine)], axis=-1
    )
    gains = [gain_self, gain_query, gain_memory, gain_mlp]
    mats = [w_qkv[0], w_self_out[0], w_query[0], w_memory[0], w_cross_out[0]]
    both = jnp.concatenate([w_fc1, w_fc2], axis=0)
    pieces = doubled(both, [1 << b for b in reversed(range(2, devices.bit_length() - 1))])
    parts = []
    fronts = [front(which[slot], window, gains, mats) for slot in range(slots)]
    taken = [[h] + [crossed(h, bits) for bits in range(1, GROUP)] for _, h in fronts]
    for slot in range(slots):
        sums = mlp(taken[slot], pieces)
        back = [crossed(sums[bits], bits) for bits in range(1, GROUP)]
        parts.append([fronts[slot][0], sums[0]] + back)
    keep, send = tail(
        which[:, 0], slot_count, side.astype(jnp.int32)[None], parts, gain_head, w_head[0], rows,
        window.shape[0],
    )
    sums = keep + passed_along(send, "side", 1).astype(jnp.float32)
    total = sums[:img_local]
    for by in range(1, WINDOW):
        piece = sums[by * img_local : (by + 1) * img_local]
        total = total + passed_along(piece.astype(jnp.bfloat16), "pairs", by).astype(jnp.float32)
    coords = total.shape[-1] * 3 // 4
    pix = total.shape[-1] // 4
    conf = jnp.maximum(total[:, :, coords:], 1.0)
    merged = [total[:, :, c * pix : (c + 1) * pix] / conf for c in range(3)]
    return jnp.concatenate(merged, axis=-1).astype(jnp.bfloat16)


def solution(mesh):
    placed = (
        P("pairs", None, "side"),
        P(),
        P("pairs", None),
        P("pairs"),
        P("side", None),
        P("side", None),
        P("side", None),
        P("side", None),
        P("side", None),
        P("side", None, None),
        P("side", None, None),
        P("side", None, None),
        P("side", None, None),
        P("side", None, None),
        P("side", "pairs", None),
        P("side", "pairs", None),
        P("side", None, None),
    )
    return jax.shard_map(
        on_device, mesh=mesh, in_specs=placed, out_specs=P("pairs", None, "side"), check_vma=False
    )
```
